128 devices in a mesh: dp: 1, ep: 128 (over z, y, x, core).
Axes of the slice: x: 4, y: 4, z: 4, core: 2. Of those that a mesh axis runs over, the one named last changes fastest.
Arguments:
- x: bfloat16 [128, 64, 2048], P(('dp', 'ep'))
- idx: int32 [128, 64, 8], P(('dp', 'ep'))
- gates: float32 [128, 64, 8], P(('dp', 'ep'))
- g1: float32 [2048], replicated
- wq: bfloat16 [2048, 4096], replicated
- wk: bfloat16 [2048, 4096], replicated
- wv: bfloat16 [2048, 4096], replicated
- wo: bfloat16 [4096, 2048], replicated
- g2: float32 [2048], replicated
- w1: bfloat16 [128, 2048, 768], P('ep')
- w3: bfloat16 [128, 2048, 768], P('ep')
- w2: bfloat16 [128, 768, 2048], P('ep')
Outputs:
- output: bfloat16 [128, 64, 2048], P(('dp', 'ep'))
All inputs are finite; a program needn't handle non-finite values.
Results may differ from the reference program's by a relative error of at most 0.0112406.
Values are sent between devices in bfloat16 or wider.
A program may use at most 1 GiB of HBM per device.

```python
import jax
import jax.numpy as jnp
from jax import lax

D = 2048
HEADS = 32
HEAD = 128
EXPERTS = 128
TOP = 8
FF = 768
SEQ = 64
SEQS = 1
EP = 128

TOK = SEQS * SEQ
AVG = TOP * TOK // EXPERTS
CAP = AVG + AVG // 2
EPS = 1e-6


def draw_routes(kk, shift):
    k1, k2, k3, k4 = jax.random.split(kk, 4)
    signs = jnp.roll(jnp.where(jnp.arange(EXPERTS) < EXPERTS // 2, 1, -1), shift)
    counts = AVG + (AVG // 2) * signs
    ends = jnp.cumsum(counts)
    ent = jnp.searchsorted(ends, jnp.arange(TOP * TOK), side='right').astype(jnp.int32)
    grid = ent.reshape(TOP, TOK).T
    grid = jnp.roll(grid, jax.random.randint(k2, (), 0, TOK), axis=0)
    gates = 2.5 * jax.nn.softmax(0.5 * jax.random.normal(k4, (TOK, TOP), jnp.float32), axis=-1)
    return grid, gates


def setup_inputs(seed: int = 0, part: int = 0) -> dict:
    kp = jax.random.fold_in(jax.random.key(seed), part)
    kx, kr = jax.random.split(kp)
    x = jax.random.normal(kx, (EP * SEQS, SEQ, D), jnp.float32).astype(jnp.bfloat16)
    shift = jax.random.randint(jax.random.fold_in(kr, 7), (), 0, EXPERTS)
    idx, gates = jax.vmap(lambda kk: draw_routes(kk, shift))(jax.random.split(kr, EP))
    ks = jax.random.split(jax.random.key(seed + 1), 9)
    wid = HEADS * HEAD

    def mat(k, shape, scale):
        return (scale * jax.random.normal(k, shape, jnp.float32)).astype(jnp.bfloat16)

    return {
        'x': x,
        'idx': idx.reshape(EP * SEQS, SEQ, TOP),
        'gates': gates.reshape(EP * SEQS, SEQ, TOP),
        'g1': jax.random.uniform(ks[0], (D,), jnp.float32, 0.5, 1.5),
        'wq': mat(ks[1], (D, wid), 1.4 * D ** -0.5),
        'wk': mat(ks[2], (D, wid), 1.4 * D ** -0.5),
        'wv': mat(ks[3], (D, wid), D ** -0.5),
        'wo': mat(ks[4], (wid, D), 2.0 * wid ** -0.5),
        'g2': jax.random.uniform(ks[5], (D,), jnp.float32, 0.5, 1.5),
        'w1': mat(ks[6], (EXPERTS, D, FF), D ** -0.5),
        'w3': mat(ks[7], (EXPERTS, D, FF), D ** -0.5),
        'w2': mat(ks[8], (EXPERTS, FF, D), FF ** -0.5),
    }


def rms(x, g):
    xf = x.astype(jnp.float32)
    return (xf * lax.rsqrt(jnp.mean(xf * xf, axis=-1, keepdims=True) + EPS) * g).astype(jnp.bfloat16)


def attend(q, k, v):
    n = q.shape[0]
    s = jnp.einsum('qhd,khd->hqk', q.astype(jnp.float32), k.astype(jnp.float32)) * HEAD ** -0.5
    mask = jnp.arange(n)[:, None] >= jnp.arange(n)[None, :]
    s = jnp.where(mask[None], s, -1e30)
    p = jax.nn.softmax(s, axis=-1).astype(jnp.bfloat16)
    o = jnp.einsum('hqk,khd->qhd', p.astype(jnp.float32), v.astype(jnp.float32))
    return o.astype(jnp.bfloat16)


def slot_pos(flat):
    n = flat.shape[0]
    order = jnp.argsort(flat, stable=True)
    se = flat[order]
    counts = jnp.zeros((EXPERTS,), jnp.int32).at[flat].add(1)
    starts = jnp.cumsum(counts) - counts
    ps = jnp.arange(n, dtype=jnp.int32) - starts[se]
    return jnp.zeros((n,), jnp.int32).at[order].set(ps)


def expert(a):
    r, a1, a3, a2 = a
    h1 = jnp.dot(r, a1, preferred_element_type=jnp.float32)
    h3 = jnp.dot(r, a3, preferred_element_type=jnp.float32)
    u = (jax.nn.silu(h1) * h3).astype(jnp.bfloat16)
    return jnp.dot(u, a2, preferred_element_type=jnp.float32).astype(jnp.bfloat16)


def reference(x, idx, gates, g1, wq, wk, wv, wo, g2, w1, w3, w2):
    n, s_len, d = x.shape
    t_all = n * s_len
    xf = x.reshape(t_all, d)
    xn = rms(xf, g1)

    def proj(w):
        return jnp.dot(xn, w, preferred_element_type=jnp.float32).astype(jnp.bfloat16).reshape(n, s_len, HEADS, HEAD)

    q = proj(wq)
    k = proj(wk)
    v = proj(wv)
    o = lax.map(lambda a: attend(a[0], a[1], a[2]), (q, k, v))
    att = jnp.dot(o.reshape(t_all, HEADS * HEAD), wo, preferred_element_type=jnp.float32).astype(jnp.bfloat16)
    h = (xf.astype(jnp.float32) + att.astype(jnp.float32)).astype(jnp.bfloat16)
    z = rms(h, g2)
    zs = z.reshape(EP, TOK, d)
    flat = idx.reshape(EP, TOK * TOP)
    dest = flat * CAP + jax.vmap(slot_pos)(flat)
    rows = jnp.repeat(zs, TOP, axis=1)
    buf = jax.vmap(lambda dd, rr: jnp.zeros((EXPERTS * CAP, d), jnp.bfloat16).at[dd].set(rr))(dest, rows)
    buf = buf.reshape(EP, EXPERTS, CAP, d).transpose(1, 0, 2, 3).reshape(EXPERTS, EP * CAP, d)
    out = lax.map(expert, (buf, w1, w3, w2))
    out = out.reshape(EXPERTS, EP, CAP, d).transpose(1, 0, 2, 3).reshape(EP, EXPERTS * CAP, d)
    got = jax.vmap(lambda oo, dd: oo[dd])(out, dest)
    got = got.reshape(t_all, TOP, d).astype(jnp.float32)
    moe = jnp.sum(got * gates.reshape(t_all, TOP, 1), axis=1)
    y = (h.astype(jnp.float32) + moe).astype(jnp.bfloat16)
    return y.reshape(n, s_len, d)
```

```python
import functools

import jax
import jax.numpy as jnp
from jax import lax
from jax.experimental import pallas as pl
from jax.experimental.pallas import tpu as pltpu
from jax.sharding import PartitionSpec as P

EPS = 1e-6
HEAD = 128
LANES = 128
MESH = pl.DeviceIdType.MESH
NBUF = 3
CHUNKS = 8
COLS = 512


def torus_axes(n):
    if n == 128:
        return ((4, 32, 1), (4, 8, 4), (4, 2, 16), (2, 1, 64))
    axes, stride = [], 1
    while stride < n:
        axes.append((2, stride, stride))
        stride *= 2
    return tuple(axes)


def peer(n, me, i, sign):
    d = 0
    for size, stride, dig in torus_axes(n):
        own = (me // stride) % size
        off = (i // dig) % size
        d = d + ((own + sign * off + size) % size) * stride
    return d


def rms(xf, g):
    return (xf * lax.rsqrt(jnp.mean(xf * xf, axis=-1, keepdims=True) + EPS) * g).astype(jnp.bfloat16)


def dotf(a, b):
    return jnp.dot(a, b, preferred_element_type=jnp.float32)


def layer_kernel(n, cap, top,
                 x_hbm, idx_hbm, gate_ref, g1_hbm, g2_hbm, wq, wk, wv, wo, w1, w3, w2,
                 y_ref,
                 xv, idxv, g1v, g2v, bq, bk, bv, bo, e1, e3, e2,
                 xn, acc, hv, tokv, dstv, toks, dsts,
                 rows32, zt, send, recv, xs, esend, back, moe32,
                 in_sem, w_sem, e_sem, s_sem, out_ssem, out_rsem, ret_ssem, ret_rsem):
    t_len, d_model = xv.shape
    kb = d_model // LANES
    wid = wq.shape[1]
    cols = bq.shape[2]
    groups = wid // cols
    per = n // CHUNKS
    rows = per * cap
    me = lax.axis_index('ep')

    def weight_copies(g, slot):
        c = pl.ds(pl.multiple_of(g * cols, cols), cols)
        return [
            pltpu.make_async_copy(wq.at[:, c], bq.at[slot], w_sem.at[slot, 0]),
            pltpu.make_async_copy(wk.at[:, c], bk.at[slot], w_sem.at[slot, 1]),
            pltpu.make_async_copy(wv.at[:, c], bv.at[slot], w_sem.at[slot, 2]),
            pltpu.make_async_copy(wo.at[c, :], bo.at[slot], w_sem.at[slot, 3]),
        ]

    ins = [
        pltpu.make_async_copy(x_hbm, xv, in_sem.at[0]),
        pltpu.make_async_copy(idx_hbm, idxv, in_sem.at[1]),
        pltpu.make_async_copy(g1_hbm, g1v, in_sem.at[2]),
        pltpu.make_async_copy(g2_hbm, g2v, in_sem.at[3]),
    ]
    for cp in ins:
        cp.start()
    for g in range(min(NBUF, groups)):
        for cp in weight_copies(g, g):
            cp.start()
    experts = [
        pltpu.make_async_copy(w1, e1, e_sem.at[0]),
        pltpu.make_async_copy(w3, e3, e_sem.at[1]),
        pltpu.make_async_copy(w2, e2, e_sem.at[2]),
    ]

    barrier = pltpu.get_barrier_semaphore()

    def hello(i, carry):
        pl.semaphore_signal(barrier, inc=1, device_id={'ep': peer(n, me, i, 1)}, device_id_type=MESH)
        return carry

    lax.fori_loop(1, n, hello, 0)

    for cp in ins:
        cp.wait()
    exp = lax.broadcasted_iota(jnp.int32, (n, t_len), 0)
    member = jnp.zeros((n, t_len), jnp.float32)
    for j in range(top):
        member = member + (idxv[j:j + 1, :] == exp).astype(jnp.float32)
    before = lax.broadcasted_iota(jnp.int32, (t_len, t_len), 0) < lax.broadcasted_iota(jnp.int32, (t_len, t_len), 1)
    pos = dotf(member.astype(jnp.bfloat16), before.astype(jnp.bfloat16))
    off = jnp.zeros((n, t_len), jnp.int32)
    for size, stride, dig in torus_axes(n):
        own = (me // stride) % size
        off = off + (((exp // stride) % size + size - own) % size) * dig
    place = (off * cap).astype(jnp.float32) + pos
    for j in range(top):
        hit = jnp.where(idxv[j:j + 1, :] == exp, place, 0.0)
        dstv[j:j + 1, :] = jnp.clip(jnp.sum(hit, axis=0, keepdims=True).astype(jnp.int32), 0, n * cap - 1)
    tok = lax.broadcasted_iota(jnp.int32, (n, t_len), 1).astype(jnp.float32)
    for c in range(cap):
        hit = jnp.where((member > 0) & (pos == c), tok, 0.0)
        tokv[:, c:c + 1] = jnp.clip(jnp.sum(hit, axis=1, keepdims=True).astype(jnp.int32), 0, t_len - 1)
    tables = [
        pltpu.make_async_copy(tokv, toks, s_sem.at[0]),
        pltpu.make_async_copy(dstv, dsts, s_sem.at[1]),
    ]
    for cp in tables:
        cp.start()

    xn[...] = rms(xv[...].astype(jnp.float32), g1v[...])
    acc[...] = jnp.zeros_like(acc)
    keep = lax.broadcasted_iota(jnp.int32, (t_len, t_len), 0) >= lax.broadcasted_iota(jnp.int32, (t_len, t_len), 1)

    def group(g, carry):
        slot = g % NBUF
        for cp in weight_copies(g, slot):
            cp.wait()
        a = xn[...]
        q = dotf(a, bq[slot]).astype(jnp.bfloat16)
        k = dotf(a, bk[slot]).astype(jnp.bfloat16)
        v = dotf(a, bv[slot]).astype(jnp.bfloat16)
        outs = []
        for hd in range(cols // HEAD):
            c = slice(hd * HEAD, (hd + 1) * HEAD)
            sc = lax.dot_general(q[:, c], k[:, c], (((1,), (1,)), ((), ())),
                                 preferred_element_type=jnp.float32) * HEAD ** -0.5
            sc = jnp.where(keep, sc, -1e30)
            ex = jnp.exp(sc - jnp.max(sc, axis=-1, keepdims=True))
            p = (ex / jnp.sum(ex, axis=-1, keepdims=True)).astype(jnp.bfloat16)
            outs.append(dotf(p, v[:, c]).astype(jnp.bfloat16))
        o = jnp.concatenate(outs, axis=1)
        acc[...] += dotf(o, bo[slot])

        @pl.when(g + NBUF < groups)
        def _():
            for cp in weight_copies(g + NBUF, slot):
                cp.start()

        @pl.when(g + NBUF == groups)
        def _():
            for cp in experts:
                cp.start()

        return carry

    lax.fori_loop(0, groups, group, 0)

    h = (xv[...].astype(jnp.float32) + acc[...].astype(jnp.bfloat16).astype(jnp.float32)).astype(jnp.bfloat16)
    hv[...] = h
    z = rms(h.astype(jnp.float32), g2v[...]).astype(jnp.float32)
    for b in range(kb):
        rows32[:t_len, b, :] = z[:, b * LANES:(b + 1) * LANES]
    zt[...] = rows32[:t_len].astype(jnp.bfloat16)
    for cp in tables:
        cp.wait()

    pl.semaphore_wait(barrier, n - 1)
    for c in range(cap):
        recv[c] = zt[toks[me, c]]

    def out_copy(i):
        blk = pl.ds(i * cap, cap)
        return pltpu.make_async_remote_copy(
            src_ref=send.at[blk], dst_ref=recv.at[blk],
            send_sem=out_ssem, recv_sem=out_rsem.at[i // per],
            device_id={'ep': peer(n, me, i, 1)}, device_id_type=MESH)

    def fill(i):
        d = peer(n, me, i, 1)
        for c in range(cap):
            send[i * cap + c] = zt[toks[d, c]]

    fill(1)

    def dispatch(i, carry):
        fill(i)
        out_copy(i - 1).start()
        return carry

    lax.fori_loop(2, n, dispatch, 0)
    out_copy(n - 1).start()

    for cp in experts:
        cp.wait()
    other = peer(n, me, 1, 1)

    def got(first, count, dst, sem):
        blk = pl.ds(first, count)
        return pltpu.make_async_remote_copy(
            src_ref=send.at[blk], dst_ref=dst.at[blk], send_sem=out_ssem, recv_sem=sem,
            device_id={'ep': other}, device_id_type=MESH)

    def ret_copy(i):
        blk = pl.ds(i * cap, cap)
        return pltpu.make_async_remote_copy(
            src_ref=esend.at[blk], dst_ref=back.at[blk],
            send_sem=ret_ssem, recv_sem=ret_rsem,
            device_id={'ep': peer(n, me, i, -1)}, device_id_type=MESH)

    def chunk(ch, carry):
        @pl.when(ch == 0)
        def _():
            got(cap, rows - cap, recv, out_rsem.at[0]).wait_recv()

        @pl.when(ch > 0)
        def _():
            got(ch * rows, rows, recv, out_rsem.at[ch]).wait_recv()

        base = ch * rows
        rows32[:rows] = recv[pl.ds(base, rows)].astype(jnp.float32)
        for b in range(kb):
            xs[:, b * LANES:(b + 1) * LANES] = rows32[:rows, b, :].astype(jnp.bfloat16)
        r = xs[...]
        h1 = dotf(r, e1[...])
        h3 = dotf(r, e3[...])
        u = (jax.nn.silu(h1) * h3).astype(jnp.bfloat16)
        eo = dotf(u, e2[...])
        for b in range(kb):
            rows32[:rows, b, :] = eo[:, b * LANES:(b + 1) * LANES]
        esend[pl.ds(base, rows)] = rows32[:rows].astype(jnp.bfloat16)

        @pl.when(ch == 0)
        def _():
            back[:cap] = esend[:cap]

        def give(b, c2):
            ret_copy(ch * per + b).start()
            return c2

        lax.fori_loop(jnp.where(ch == 0, 1, 0), per, give, 0)
        return carry

    lax.fori_loop(0, CHUNKS, chunk, 0)

    whole = pl.ds(cap, (n - 1) * cap)
    tail = pltpu.make_async_remote_copy(
        src_ref=esend.at[whole], dst_ref=back.at[whole], send_sem=ret_ssem, recv_sem=ret_rsem,
        device_id={'ep': other}, device_id_type=MESH)
    tail.wait_recv()

    def combine(t, carry):
        total = jnp.zeros((kb, LANES), jnp.float32)
        for j in range(top):
            total = total + back[dsts[j, t]].astype(jnp.float32) * gate_ref[j, t]
        moe32[t] = total
        return carry

    lax.fori_loop(0, t_len, combine, 0)
    for b in range(kb):
        c = slice(b * LANES, (b + 1) * LANES)
        y_ref[:, c] = (hv[:, c].astype(jnp.float32) + moe32[:, b, :]).astype(jnp.bfloat16)

    pltpu.make_async_remote_copy(
        src_ref=send.at[whole], dst_ref=recv.at[whole], send_sem=out_ssem, recv_sem=ret_rsem,
        device_id={'ep': other}, device_id_type=MESH).wait_send()
    tail.wait_send()


def layer(n, x, idx, gates, g1, g2, wq, wk, wv, wo, w1, w3, w2):
    t_len, d = x.shape
    top = idx.shape[0]
    avg = top * t_len // n
    cap = avg + avg // 2
    cols = min(COLS, wq.shape[1])
    kb = d // LANES
    ff = w1.shape[1]
    per = n // CHUNKS
    rows = per * cap
    bf, f32, i32 = jnp.bfloat16, jnp.float32, jnp.int32
    anyspec = pl.BlockSpec(memory_space=pl.ANY)
    V, DMA = pltpu.VMEM, pltpu.SemaphoreType.DMA
    return pl.pallas_call(
        functools.partial(layer_kernel, n, cap, top),
        out_shape=jax.ShapeDtypeStruct((t_len, d), bf),
        in_specs=[anyspec, anyspec, pl.BlockSpec(memory_space=pltpu.SMEM)] + [anyspec] * 9,
        out_specs=pl.BlockSpec(memory_space=pltpu.VMEM),
        scratch_shapes=[
            V((t_len, d), bf), V((top, t_len), i32), V((1, d), f32), V((1, d), f32),
            V((NBUF, d, cols), bf), V((NBUF, d, cols), bf), V((NBUF, d, cols), bf), V((NBUF, cols, d), bf),
            V((d, ff), bf), V((d, ff), bf), V((ff, d), bf),
            V((t_len, d), bf), V((t_len, d), f32), V((t_len, d), bf),
            V((n, cap), i32), V((top, t_len), i32), pltpu.SMEM((n, cap), i32), pltpu.SMEM((top, t_len), i32),
            V((max(rows, t_len), kb, LANES), f32), V((t_len, kb, LANES), bf),
            V((n * cap, kb, LANES), bf), V((n * cap, kb, LANES), bf), V((rows, d), bf),
            V((n * cap, kb, LANES), bf), V((n * cap, kb, LANES), bf), V((t_len, kb, LANES), f32),
            DMA((4,)), DMA((NBUF, 4)), DMA((3,)), DMA((2,)), DMA, DMA((CHUNKS,)), DMA, DMA,
        ],
        compiler_params=pltpu.CompilerParams(
            collective_id=0, has_side_effects=True, vmem_limit_bytes=67043328),
        name='layer',
    )(x, idx, gates, g1, g2, wq, wk, wv, wo, w1, w3, w2)


def solution(mesh):
    n = mesh.shape['ep']
    tok = P(('dp', 'ep'))
    rep = P()
    exs = P('ep')

    def body(x, idx, gates, g1, wq, wk, wv, wo, g2, w1, w3, w2):
        d = x.shape[-1]
        y = layer(n, x[0], idx[0].T, gates[0].T, g1.reshape(1, d), g2.reshape(1, d),
                  wq, wk, wv, wo, w1[0], w3[0], w2[0])
        return y[None]

    return jax.shard_map(body, mesh=mesh, in_specs=(tok, tok, tok, rep, rep, rep, rep, rep, rep, exs, exs, exs), out_specs=tok, check_vma=False)
```

```python
import functools

import jax
import jax.numpy as jnp
from jax import lax
from jax.experimental import pallas as pl
from jax.experimental.pallas import tpu as pltpu
from jax.sharding import PartitionSpec as P

EPS = 1e-6
HEAD = 128
LANES = 128
MESH = pl.DeviceIdType.MESH
NBUF = 3
CHUNKS = 8
COLS = 512


def torus_axes(n):
    if n == 128:
        return ((4, 32), (4, 8), (4, 2), (2, 1))
    axes, stride = [], 1
    while stride < n:
        axes.append((2, stride))
        stride *= 2
    return tuple(axes)


def steps(n, i):
    axes = torus_axes(n)
    out, div = [], 1
    for size, _ in axes:
        out.append((i // div + (i if div > 1 else 0)) % size)
        div *= size
    return out


def number(n, deltas):
    axes = torus_axes(n)
    i, div = deltas[0], axes[0][0]
    for (size, _), d in zip(axes[1:], deltas[1:]):
        low = i
        i = i + ((d - low % size + size) % size) * div
        div *= size
    return i


def peer(n, me, i, sign):
    d = 0
    for (size, stride), off in zip(torus_axes(n), steps(n, i)):
        own = (me // stride) % size
        d = d + ((own + sign * off + size) % size) * stride
    return d


def rms(xf, g):
    return (xf * lax.rsqrt(jnp.mean(xf * xf, axis=-1, keepdims=True) + EPS) * g).astype(jnp.bfloat16)


def dotf(a, b):
    return jnp.dot(a, b, preferred_element_type=jnp.float32)


def layer_kernel(n, cap, top,
                 x_hbm, xp_hbm, idx_hbm, gate_ref, g1_hbm, g2_hbm, wq, wk, wv, wo, w1, w3, w2,
                 y_ref,
                 xv, idxv, g1v, g2v, bq, bk, bv, bo, e1, e3, e2,
                 xn, acc, part, hv, tokv, dstv, toks, dsts,
                 rows32, zt, send, recv, xs, esend, back, moe32,
                 in_sem, w_sem, e_sem, s_sem, p_ssem, p_rsem, out_ssem, out_rsem, ret_ssem, ret_rsem):
    t2, d_model = xv.shape
    t_len = t2 // 2
    kb = d_model // LANES
    wid = wq.shape[1]
    cols = bq.shape[2]
    groups = wid // 2 // cols
    per = n // CHUNKS
    rows = per * cap
    me = lax.axis_index('ep')
    core = me % 2
    mate = me + 1 - 2 * core

    def weight_copies(g, slot):
        c = pl.ds(pl.multiple_of((core * groups + g) * cols, cols), cols)
        return [
            pltpu.make_async_copy(wq.at[:, c], bq.at[slot], w_sem.at[slot, 0]),
            pltpu.make_async_copy(wk.at[:, c], bk.at[slot], w_sem.at[slot, 1]),
            pltpu.make_async_copy(wv.at[:, c], bv.at[slot], w_sem.at[slot, 2]),
            pltpu.make_async_copy(wo.at[c, :], bo.at[slot], w_sem.at[slot, 3]),
        ]

    ins = [
        pltpu.make_async_copy(x_hbm, xv.at[:t_len], in_sem.at[0]),
        pltpu.make_async_copy(xp_hbm, xv.at[t_len:], in_sem.at[4]),
        pltpu.make_async_copy(idx_hbm, idxv, in_sem.at[1]),
        pltpu.make_async_copy(g1_hbm, g1v, in_sem.at[2]),
        pltpu.make_async_copy(g2_hbm, g2v, in_sem.at[3]),
    ]
    for cp in ins:
        cp.start()
    for g in range(min(NBUF, groups)):
        for cp in weight_copies(g, g):
            cp.start()
    experts = [
        pltpu.make_async_copy(w1, e1, e_sem.at[0]),
        pltpu.make_async_copy(w3, e3, e_sem.at[1]),
        pltpu.make_async_copy(w2, e2, e_sem.at[2]),
    ]

    barrier = pltpu.get_barrier_semaphore()

    def hello(i, carry):
        pl.semaphore_signal(barrier, inc=1, device_id={'ep': peer(n, me, i, 1)}, device_id_type=MESH)
        return carry

    lax.fori_loop(1, n, hello, 0)

    for cp in ins:
        cp.wait()
    exp = lax.broadcasted_iota(jnp.int32, (n, t_len), 0)
    member = jnp.zeros((n, t_len), jnp.float32)
    for j in range(top):
        member = member + (idxv[j:j + 1, :] == exp).astype(jnp.float32)
    before = lax.broadcasted_iota(jnp.int32, (t_len, t_len), 0) < lax.broadcasted_iota(jnp.int32, (t_len, t_len), 1)
    pos = dotf(member.astype(jnp.bfloat16), before.astype(jnp.bfloat16))
    off = number(n, [((exp // stride) % size + size - (me // stride) % size) % size
                     for size, stride in torus_axes(n)])
    place = (off * cap).astype(jnp.float32) + pos
    for j in range(top):
        hit = jnp.where(idxv[j:j + 1, :] == exp, place, 0.0)
        dstv[j:j + 1, :] = jnp.clip(jnp.sum(hit, axis=0, keepdims=True).astype(jnp.int32), 0, n * cap - 1)
    tok = lax.broadcasted_iota(jnp.int32, (n, t_len), 1).astype(jnp.float32)
    for c in range(cap):
        hit = jnp.where((member > 0) & (pos == c), tok, 0.0)
        tokv[:, c:c + 1] = jnp.clip(jnp.sum(hit, axis=1, keepdims=True).astype(jnp.int32), 0, t_len - 1)
    tables = [
        pltpu.make_async_copy(tokv, toks, s_sem.at[0]),
        pltpu.make_async_copy(dstv, dsts, s_sem.at[1]),
    ]
    for cp in tables:
        cp.start()

    xn[...] = rms(xv[...].astype(jnp.float32), g1v[...])
    acc[...] = jnp.zeros_like(acc)
    row = lax.broadcasted_iota(jnp.int32, (t2, t2), 0)
    col = lax.broadcasted_iota(jnp.int32, (t2, t2), 1)
    keep = (row >= col) & (row // t_len == col // t_len)

    def group(g, carry):
        slot = g % NBUF
        for cp in weight_copies(g, slot):
            cp.wait()
        a = xn[...]
        q = dotf(a, bq[slot]).astype(jnp.bfloat16)
        k = dotf(a, bk[slot]).astype(jnp.bfloat16)
        v = dotf(a, bv[slot]).astype(jnp.bfloat16)
        outs = []
        for hd in range(cols // HEAD):
            c = slice(hd * HEAD, (hd + 1) * HEAD)
            sc = lax.dot_general(q[:, c], k[:, c], (((1,), (1,)), ((), ())),
                                 preferred_element_type=jnp.float32) * HEAD ** -0.5
            sc = jnp.where(keep, sc, -1e30)
            ex = jnp.exp(sc - jnp.max(sc, axis=-1, keepdims=True))
            p = (ex / jnp.sum(ex, axis=-1, keepdims=True)).astype(jnp.bfloat16)
            outs.append(dotf(p, v[:, c]).astype(jnp.bfloat16))
        o = jnp.concatenate(outs, axis=1)
        acc[...] += dotf(o, bo[slot])

        @pl.when(g + NBUF < groups)
        def _():
            for cp in weight_copies(g + NBUF, slot):
                cp.start()

        @pl.when(g + NBUF == groups)
        def _():
            for cp in experts:
                cp.start()

        return carry

    lax.fori_loop(0, groups, group, 0)

    pl.semaphore_wait(barrier, n - 1)
    swap = pltpu.make_async_remote_copy(
        src_ref=acc.at[t_len:], dst_ref=part, send_sem=p_ssem, recv_sem=p_rsem,
        device_id={'ep': mate}, device_id_type=MESH)
    swap.start()
    swap.wait()
    att = (acc[:t_len] + part[...]).astype(jnp.bfloat16)
    h = (xv[:t_len].astype(jnp.float32) + att.astype(jnp.float32)).astype(jnp.bfloat16)
    hv[...] = h
    z = rms(h.astype(jnp.float32), g2v[...]).astype(jnp.float32)
    for b in range(kb):
        rows32[:t_len, b, :] = z[:, b * LANES:(b + 1) * LANES]
    zt[...] = rows32[:t_len].astype(jnp.bfloat16)
    for cp in tables:
        cp.wait()

    for c in range(cap):
        recv[c] = zt[toks[me, c]]

    def out_copy(i):
        blk = pl.ds(i * cap, cap)
        return pltpu.make_async_remote_copy(
            src_ref=send.at[blk], dst_ref=recv.at[blk],
            send_sem=out_ssem, recv_sem=out_rsem.at[i // per],
            device_id={'ep': peer(n, me, i, 1)}, device_id_type=MESH)

    def fill(i):
        d = peer(n, me, i, 1)
        for c in range(cap):
            send[i * cap + c] = zt[toks[d, c]]

    fill(1)

    def dispatch(i, carry):
        fill(i)
        out_copy(i - 1).start()
        return carry

    lax.fori_loop(2, n, dispatch, 0)
    out_copy(n - 1).start()

    for cp in experts:
        cp.wait()
    other = peer(n, me, 1, 1)

    def got(first, count, dst, sem):
        blk = pl.ds(first, count)
        return pltpu.make_async_remote_copy(
            src_ref=send.at[blk], dst_ref=dst.at[blk], send_sem=out_ssem, recv_sem=sem,
            device_id={'ep': other}, device_id_type=MESH)

    def ret_copy(i):
        blk = pl.ds(i * cap, cap)
        return pltpu.make_async_remote_copy(
            src_ref=esend.at[blk], dst_ref=back.at[blk],
            send_sem=ret_ssem, recv_sem=ret_rsem,
            device_id={'ep': peer(n, me, i, -1)}, device_id_type=MESH)

    def chunk(ch, carry):
        @pl.when(ch == 0)
        def _():
            got(cap, rows - cap, recv, out_rsem.at[0]).wait_recv()

        @pl.when(ch > 0)
        def _():
            got(ch * rows, rows, recv, out_rsem.at[ch]).wait_recv()

        base = ch * rows
        rows32[:rows] = recv[pl.ds(base, rows)].astype(jnp.float32)
        for b in range(kb):
            xs[:, b * LANES:(b + 1) * LANES] = rows32[:rows, b, :].astype(jnp.bfloat16)
        r = xs[...]
        h1 = dotf(r, e1[...])
        h3 = dotf(r, e3[...])
        u = (jax.nn.silu(h1) * h3).astype(jnp.bfloat16)
        eo = dotf(u, e2[...])
        for b in range(kb):
            rows32[:rows, b, :] = eo[:, b * LANES:(b + 1) * LANES]
        esend[pl.ds(base, rows)] = rows32[:rows].astype(jnp.bfloat16)

        @pl.when(ch == 0)
        def _():
            back[:cap] = esend[:cap]

        def give(b, c2):
            ret_copy(ch * per + b).start()
            return c2

        lax.fori_loop(jnp.where(ch == 0, 1, 0), per, give, 0)
        return carry

    lax.fori_loop(0, CHUNKS, chunk, 0)

    whole = pl.ds(cap, (n - 1) * cap)
    tail = pltpu.make_async_remote_copy(
        src_ref=esend.at[whole], dst_ref=back.at[whole], send_sem=ret_ssem, recv_sem=ret_rsem,
        device_id={'ep': other}, device_id_type=MESH)
    tail.wait_recv()

    def combine(t, carry):
        total = jnp.zeros((kb, LANES), jnp.float32)
        for j in range(top):
            total = total + back[dsts[j, t]].astype(jnp.float32) * gate_ref[j, t]
        moe32[t] = total
        return carry

    lax.fori_loop(0, t_len, combine, 0)
    for b in range(kb):
        c = slice(b * LANES, (b + 1) * LANES)
        y_ref[:, c] = (hv[:, c].astype(jnp.float32) + moe32[:, b, :]).astype(jnp.bfloat16)

    pltpu.make_async_remote_copy(
        src_ref=send.at[whole], dst_ref=recv.at[whole], send_sem=out_ssem, recv_sem=ret_rsem,
        device_id={'ep': other}, device_id_type=MESH).wait_send()
    tail.wait_send()


def layer(n, x, xp, idx, gates, g1, g2, wq, wk, wv, wo, w1, w3, w2):
    t_len, d = x.shape
    top = idx.shape[0]
    avg = top * t_len // n
    cap = avg + avg // 2
    cols = min(COLS, wq.shape[1] // 2)
    kb = d // LANES
    ff = w1.shape[1]
    per = n // CHUNKS
    rows = per * cap
    bf, f32, i32 = jnp.bfloat16, jnp.float32, jnp.int32
    anyspec = pl.BlockSpec(memory_space=pl.ANY)
    V, DMA = pltpu.VMEM, pltpu.SemaphoreType.DMA
    return pl.pallas_call(
        functools.partial(layer_kernel, n, cap, top),
        out_shape=jax.ShapeDtypeStruct((t_len, d), bf),
        in_specs=[anyspec, anyspec, anyspec, pl.BlockSpec(memory_space=pltpu.SMEM)] + [anyspec] * 9,
        out_specs=pl.BlockSpec(memory_space=pltpu.VMEM),
        scratch_shapes=[
            V((2 * t_len, d), bf), V((top, t_len), i32), V((1, d), f32), V((1, d), f32),
            V((NBUF, d, cols), bf), V((NBUF, d, cols), bf), V((NBUF, d, cols), bf), V((NBUF, cols, d), bf),
            V((d, ff), bf), V((d, ff), bf), V((ff, d), bf),
            V((2 * t_len, d), bf), V((2 * t_len, d), f32), V((t_len, d), f32), V((t_len, d), bf),
            V((n, cap), i32), V((top, t_len), i32), pltpu.SMEM((n, cap), i32), pltpu.SMEM((top, t_len), i32),
            V((max(rows, t_len), kb, LANES), f32), V((t_len, kb, LANES), bf),
            V((n * cap, kb, LANES), bf), V((n * cap, kb, LANES), bf), V((rows, d), bf),
            V((n * cap, kb, LANES), bf), V((n * cap, kb, LANES), bf), V((t_len, kb, LANES), f32),
            DMA((5,)), DMA((NBUF, 4)), DMA((3,)), DMA((2,)), DMA, DMA, DMA, DMA((CHUNKS,)), DMA, DMA,
        ],
        compiler_params=pltpu.CompilerParams(
            collective_id=0, has_side_effects=True, vmem_limit_bytes=67043328),
        name='layer',
    )(x, xp, idx, gates, g1, g2, wq, wk, wv, wo, w1, w3, w2)


def solution(mesh):
    n = mesh.shape['ep']
    tok = P(('dp', 'ep'))
    rep = P()
    exs = P('ep')

    def body(x, idx, gates, g1, wq, wk, wv, wo, g2, w1, w3, w2):
        d = x.shape[-1]
        xp = lax.ppermute(x[0], 'ep', [(i, i ^ 1) for i in range(n)])
        y = layer(n, x[0], xp, idx[0].T, gates[0].T, g1.reshape(1, d), g2.reshape(1, d),
                  wq, wk, wv, wo, w1[0], w3[0], w2[0])
        return y[None]

    return jax.shard_map(body, mesh=mesh, in_specs=(tok, tok, tok, rep, rep, rep, rep, rep, rep, exs, exs, exs), out_specs=tok, check_vma=False)
```

```python
import functools

import jax
import jax.numpy as jnp
from jax import lax
from jax.experimental import pallas as pl
from jax.experimental.pallas import tpu as pltpu
from jax.sharding import PartitionSpec as P

EPS = 1e-6
HEAD = 128
LANES = 128
MESH = pl.DeviceIdType.MESH
NBUF = 4
PAIR = 2
PARTS = 2
COLS = 512


def torus_axes(n):
    if n == 128:
        return ((4, 32), (4, 8), (4, 2), (2, 1))
    axes, stride = [], 1
    while stride < n:
        axes.append((2, stride))
        stride *= 2
    return tuple(axes)


def number(n, deltas):
    axes = torus_axes(n)
    i, div = deltas[0], axes[0][0]
    for (size, _), d in zip(axes[1:], deltas[1:]):
        low = i
        i = i + ((d - low % size + size) % size) * div
        div *= size
    return i


def peer(n, own, q, a, sign):
    axes = torus_axes(n)
    d, div = 0, 1
    for k, (size, stride) in enumerate(axes):
        step = a if k == 0 else lax.rem(lax.div(q, div) + a, size)
        d = d + lax.rem(own[k] + sign * step + size, size) * stride
        div *= size if k else 1
    return d


def rms(xf, g):
    return (xf * lax.rsqrt(jnp.mean(xf * xf, axis=-1, keepdims=True) + EPS) * g).astype(jnp.bfloat16)


def dotf(a, b):
    return jnp.dot(a, b, preferred_element_type=jnp.float32)


def layer_kernel(n, cap, top,
                 x_hbm, xp_hbm, idx_hbm, gate_ref, g1_hbm, g2_hbm, wq, wk, wv, wo, w1, w3, w2,
                 hv, moe_ref,
                 xv, idxv, g1v, g2v, bq, bk, bv, bo, e1, e3, e2,
                 xn, acc, part, tokv, dstv, toks, dsts,
                 rows32, zt, send, recv, xs, esend, back, moe32,
                 in_sem, w_sem, e_sem, s_sem, p_ssem, p_rsem, out_ssem, out_rsem, ret_ssem, ret_rsem):
    t2, d_model = xv.shape
    t_len = t2 // 2
    kb = d_model // LANES
    wid = wq.shape[1]
    cols = bq.shape[2]
    groups = wid // 2 // cols
    passes = cap // PAIR
    per = n // PARTS
    rows = per * PAIR
    first = torus_axes(n)[0][0]
    me = lax.axis_index('ep')
    own = [lax.rem(lax.div(me, stride), size) for size, stride in torus_axes(n)]
    core = lax.rem(me, 2)
    mate = me + 1 - 2 * core

    def weight_copies(g, slot):
        c = pl.ds(pl.multiple_of((core * groups + g) * cols, cols), cols)
        return [
            pltpu.make_async_copy(wq.at[:, c], bq.at[slot], w_sem.at[slot, 0]),
            pltpu.make_async_copy(wk.at[:, c], bk.at[slot], w_sem.at[slot, 1]),
            pltpu.make_async_copy(wv.at[:, c], bv.at[slot], w_sem.at[slot, 2]),
            pltpu.make_async_copy(wo.at[c, :], bo.at[slot], w_sem.at[slot, 3]),
        ]

    ins = [
        pltpu.make_async_copy(x_hbm, xv.at[:t_len], in_sem.at[0]),
        pltpu.make_async_copy(xp_hbm, xv.at[t_len:], in_sem.at[4]),
        pltpu.make_async_copy(idx_hbm, idxv, in_sem.at[1]),
        pltpu.make_async_copy(g1_hbm, g1v, in_sem.at[2]),
        pltpu.make_async_copy(g2_hbm, g2v, in_sem.at[3]),
    ]
    for cp in ins:
        cp.start()
    for g in range(min(NBUF, groups)):
        for cp in weight_copies(g, g):
            cp.start()
    experts = [
        pltpu.make_async_copy(w1, e1, e_sem.at[0]),
        pltpu.make_async_copy(w3, e3, e_sem.at[1]),
        pltpu.make_async_copy(w2, e2, e_sem.at[2]),
    ]

    barrier = pltpu.get_barrier_semaphore()

    def hello(j, carry):
        pl.semaphore_signal(barrier, inc=1, device_id={'ep': j}, device_id_type=MESH)
        return carry

    lax.fori_loop(me + 1, n, hello, 0)
    lax.fori_loop(0, me, hello, 0)

    for cp in ins:
        cp.wait()
    exp = lax.broadcasted_iota(jnp.int32, (n, t_len), 0)
    member = jnp.zeros((n, t_len), jnp.float32)
    for j in range(top):
        member = member + (idxv[j:j + 1, :] == exp).astype(jnp.float32)
    before = lax.broadcasted_iota(jnp.int32, (t_len, t_len), 0) < lax.broadcasted_iota(jnp.int32, (t_len, t_len), 1)
    pos = dotf(member.astype(jnp.bfloat16), before.astype(jnp.bfloat16))
    off = number(n, [((exp // stride) % size + size - (me // stride) % size) % size
                     for size, stride in torus_axes(n)])
    nth = pos.astype(jnp.int32)
    place = (((nth // PAIR) * n + off) * PAIR + nth % PAIR).astype(jnp.float32)
    for j in range(top):
        hit = jnp.where(idxv[j:j + 1, :] == exp, place, 0.0)
        dstv[j:j + 1, :] = jnp.clip(jnp.sum(hit, axis=0, keepdims=True).astype(jnp.int32), 0, n * cap - 1)
    tok = lax.broadcasted_iota(jnp.int32, (n, t_len), 1).astype(jnp.float32)
    for c in range(cap):
        hit = jnp.where((member > 0) & (pos == c), tok, 0.0)
        tokv[:, c:c + 1] = jnp.clip(jnp.sum(hit, axis=1, keepdims=True).astype(jnp.int32), 0, t_len - 1)
    tables = [
        pltpu.make_async_copy(tokv, toks, s_sem.at[0]),
        pltpu.make_async_copy(dstv, dsts, s_sem.at[1]),
    ]
    for cp in tables:
        cp.start()

    xn[...] = rms(xv[...].astype(jnp.float32), g1v[...])
    acc[...] = jnp.zeros_like(acc)
    row = lax.broadcasted_iota(jnp.int32, (t2, t2), 0)
    col = lax.broadcasted_iota(jnp.int32, (t2, t2), 1)
    keep = (row >= col) & (row // t_len == col // t_len)

    def group(g, carry):
        slot = g % NBUF
        for cp in weight_copies(g, slot):
            cp.wait()
        a = xn[...]
        q = dotf(a, bq[slot]).astype(jnp.bfloat16)
        k = dotf(a, bk[slot]).astype(jnp.bfloat16)
        v = dotf(a, bv[slot]).astype(jnp.bfloat16)
        outs = []
        for hd in range(cols // HEAD):
            c = slice(hd * HEAD, (hd + 1) * HEAD)
            sc = lax.dot_general(q[:, c], k[:, c], (((1,), (1,)), ((), ())),
                                 preferred_element_type=jnp.float32) * HEAD ** -0.5
            sc = jnp.where(keep, sc, -1e30)
            ex = jnp.exp(sc - jnp.max(sc, axis=-1, keepdims=True))
            p = (ex / jnp.sum(ex, axis=-1, keepdims=True)).astype(jnp.bfloat16)
            outs.append(dotf(p, v[:, c]).astype(jnp.bfloat16))
        o = jnp.concatenate(outs, axis=1)
        acc[...] += dotf(o, bo[slot])

        @pl.when(g + NBUF < groups)
        def _():
            for cp in weight_copies(g + NBUF, slot):
                cp.start()

        @pl.when(g == max(groups - 2, 0))
        def _():
            for cp in experts:
                cp.start()

        return carry

    lax.fori_loop(0, groups, group, 0)

    pl.semaphore_wait(barrier, n - 1)
    swap = pltpu.make_async_remote_copy(
        src_ref=acc.at[t_len:], dst_ref=part, send_sem=p_ssem, recv_sem=p_rsem,
        device_id={'ep': mate}, device_id_type=MESH)
    swap.start()
    swap.wait()
    att = (acc[:t_len] + part[...]).astype(jnp.bfloat16)
    h = (xv[:t_len].astype(jnp.float32) + att.astype(jnp.float32)).astype(jnp.bfloat16)
    hv[...] = h
    z = rms(h.astype(jnp.float32), g2v[...]).astype(jnp.float32)
    for b in range(kb):
        rows32[:t_len, b, :] = z[:, b * LANES:(b + 1) * LANES]
    zt[...] = rows32[:t_len].astype(jnp.bfloat16)
    for cp in tables:
        cp.wait()

    for p in range(passes):
        for c in range(PAIR):
            recv[p * n * PAIR + c] = zt[toks[me, p * PAIR + c]]

    def block(p, i):
        return pl.ds((p * n + i) * PAIR, PAIR)

    def fill(p, q, a):
        d = peer(n, own, q, a, 1)
        for c in range(PAIR):
            send[(p * n + first * q + a) * PAIR + c] = zt[toks[d, p * PAIR + c]]

    def out_copy(p, q, a):
        i = first * q + a
        return pltpu.make_async_remote_copy(
            src_ref=send.at[block(p, i)], dst_ref=recv.at[block(p, i)],
            send_sem=out_ssem.at[p], recv_sem=out_rsem.at[p * PARTS + lax.div(i, per)],
            device_id={'ep': peer(n, own, q, a, 1)}, device_id_type=MESH)

    quads = n // first
    for p in range(passes):
        for a in range(first):
            fill(p, 0, a)

        def dispatch(q, carry):
            for a in range(first):
                fill(p, q, a)
            for a in range(first):
                if a == 0:
                    @pl.when(q > 1)
                    def _():
                        out_copy(p, q - 1, a).start()
                else:
                    out_copy(p, q - 1, a).start()
            return carry

        lax.fori_loop(1, quads, dispatch, 0)
        for a in range(first):
            out_copy(p, quads - 1, a).start()

    for cp in experts:
        cp.wait()

    def span(lo, count, src, dst, ssem, rsem):
        blk = pl.ds(lo, count)
        return pltpu.make_async_remote_copy(
            src_ref=src.at[blk], dst_ref=dst.at[blk], send_sem=ssem, recv_sem=rsem,
            device_id={'ep': mate}, device_id_type=MESH)

    def ret_copy(p, q, a):
        i = first * q + a
        return pltpu.make_async_remote_copy(
            src_ref=esend.at[block(p, i)], dst_ref=back.at[block(p, i)],
            send_sem=ret_ssem.at[p], recv_sem=ret_rsem.at[p],
            device_id={'ep': peer(n, own, q, a, -1)}, device_id_type=MESH)

    def chunk(ch, carry):
        p = lax.div(ch, PARTS)
        half = lax.rem(ch, PARTS)
        base = ch * rows

        @pl.when(half == 0)
        def _():
            span(base + PAIR, rows - PAIR, send, recv, out_ssem.at[0], out_rsem.at[ch]).wait_recv()

        @pl.when(half > 0)
        def _():
            span(base, rows, send, recv, out_ssem.at[0], out_rsem.at[ch]).wait_recv()

        rows32[:rows] = recv[pl.ds(base, rows)].astype(jnp.float32)
        for b in range(kb):
            xs[:, b * LANES:(b + 1) * LANES] = rows32[:rows, b, :].astype(jnp.bfloat16)
        r = xs[...]
        h1 = dotf(r, e1[...])
        h3 = dotf(r, e3[...])
        u = (jax.nn.silu(h1) * h3).astype(jnp.bfloat16)
        eo = dotf(u, e2[...])
        for b in range(kb):
            rows32[:rows, b, :] = eo[:, b * LANES:(b + 1) * LANES]
        esend[pl.ds(base, rows)] = rows32[:rows].astype(jnp.bfloat16)

        @pl.when(half == 0)
        def _():
            back[pl.ds(base, PAIR)] = esend[pl.ds(base, PAIR)]

        def give(k, c2):
            q = half * (quads // PARTS) + k
            for a in range(first):
                if a == 0:
                    @pl.when(q > 0)
                    def _():
                        ret_copy(p, q, a).start()
                else:
                    ret_copy(p, q, a).start()
            return c2

        lax.fori_loop(0, quads // PARTS, give, 0)
        return carry

    lax.fori_loop(0, passes * PARTS, chunk, 0)

    def full(p, src, dst, ssem, rsem):
        return span((p * n + 1) * PAIR, (n - 1) * PAIR, src, dst, ssem, rsem)

    for p in range(passes):
        full(p, esend, back, ret_ssem.at[p], ret_rsem.at[p]).wait_recv()

    def combine(t, carry):
        total = jnp.zeros((kb, LANES), jnp.float32)
        for j in range(top):
            total = total + back[dsts[j, t]].astype(jnp.float32) * gate_ref[j, t]
        moe32[t] = total
        return carry

    lax.fori_loop(0, t_len, combine, 0)
    for b in range(kb):
        moe_ref[:, b * LANES:(b + 1) * LANES] = moe32[:, b, :]

    for p in range(passes):
        full(p, send, recv, out_ssem.at[p], out_rsem.at[0]).wait_send()
        full(p, esend, back, ret_ssem.at[p], ret_rsem.at[p]).wait_send()


def layer(n, x, xp, idx, gates, g1, g2, wq, wk, wv, wo, w1, w3, w2):
    t_len, d = x.shape
    top = idx.shape[0]
    avg = top * t_len // n
    cap = avg + avg // 2
    cols = min(COLS, wq.shape[1] // 2)
    kb = d // LANES
    ff = w1.shape[1]
    passes = cap // PAIR
    rows = n // PARTS * PAIR
    bf, f32, i32 = jnp.bfloat16, jnp.float32, jnp.int32
    anyspec = pl.BlockSpec(memory_space=pl.ANY)
    V, DMA = pltpu.VMEM, pltpu.SemaphoreType.DMA
    return pl.pallas_call(
        functools.partial(layer_kernel, n, cap, top),
        out_shape=(jax.ShapeDtypeStruct((t_len, d), bf), jax.ShapeDtypeStruct((t_len, d), f32)),
        in_specs=[anyspec, anyspec, anyspec, pl.BlockSpec(memory_space=pltpu.SMEM)] + [anyspec] * 9,
        out_specs=(pl.BlockSpec(memory_space=pltpu.VMEM), pl.BlockSpec(memory_space=pltpu.VMEM)),
        scratch_shapes=[
            V((2 * t_len, d), bf), V((top, t_len), i32), V((1, d), f32), V((1, d), f32),
            V((NBUF, d, cols), bf), V((NBUF, d, cols), bf), V((NBUF, d, cols), bf), V((NBUF, cols, d), bf),
            V((d, ff), bf), V((d, ff), bf), V((ff, d), bf),
            V((2 * t_len, d), bf), V((2 * t_len, d), f32), V((t_len, d), f32),
            V((n, cap), i32), V((top, t_len), i32), pltpu.SMEM((n, cap), i32), pltpu.SMEM((top, t_len), i32),
            V((max(rows, t_len), kb, LANES), f32), V((t_len, kb, LANES), bf),
            V((n * cap, kb, LANES), bf), V((n * cap, kb, LANES), bf), V((rows, d), bf),
            V((n * cap, kb, LANES), bf), V((n * cap, kb, LANES), bf), V((t_len, kb, LANES), f32),
            DMA((5,)), DMA((NBUF, 4)), DMA((3,)), DMA((2,)), DMA, DMA,
            DMA((passes,)), DMA((passes * PARTS,)), DMA((passes,)), DMA((passes,)),
        ],
        compiler_params=pltpu.CompilerParams(
            collective_id=0, has_side_effects=True, vmem_limit_bytes=67043328),
        name='layer',
    )(x, xp, idx, gates, g1, g2, wq, wk, wv, wo, w1, w3, w2)


def solution(mesh):
    n = mesh.shape['ep']
    tok = P(('dp', 'ep'))
    rep = P()
    exs = P('ep')

    def body(x, idx, gates, g1, wq, wk, wv, wo, g2, w1, w3, w2):
        d = x.shape[-1]
        xp = lax.ppermute(x[0], 'ep', [(i, i ^ 1) for i in range(n)])
        h, moe = layer(n, x[0], xp, idx[0].T, gates[0].T, g1.reshape(1, d), g2.reshape(1, d),
                  wq, wk, wv, wo, w1[0], w3[0], w2[0])
        return (h.astype(jnp.float32) + moe).astype(jnp.bfloat16)[None]

    return jax.shard_map(body, mesh=mesh, in_specs=(tok, tok, tok, rep, rep, rep, rep, rep, rep, exs, exs, exs), out_specs=tok, check_vma=False)
```

```python
import functools

import jax
import jax.numpy as jnp
from jax import lax
from jax.experimental import pallas as pl
from jax.experimental.pallas import tpu as pltpu
from jax.sharding import PartitionSpec as P

EPS = 1e-6
HEAD = 128
LANES = 128
MESH = pl.DeviceIdType.MESH
NBUF = 4
PAIR = 2
PARTS = 2
COLS = 512


def torus_axes(n):
    if n == 128:
        return ((4, 32), (4, 8), (4, 2), (2, 1))
    axes, stride = [], 1
    while stride < n:
        axes.append((2, stride))
        stride *= 2
    return tuple(axes)


def number(n, deltas):
    axes = torus_axes(n)
    i, div = deltas[0], axes[0][0]
    for (size, _), d in zip(axes[1:], deltas[1:]):
        low = i
        i = i + ((d - low % size + size) % size) * div
        div *= size
    return i


def peer(n, own, q, a, sign):
    axes = torus_axes(n)
    d, div = 0, 1
    for k, (size, stride) in enumerate(axes):
        step = a if k == 0 else lax.rem(lax.div(q, div) + a, size)
        d = d + lax.rem(own[k] + sign * step + size, size) * stride
        div *= size if k else 1
    return d


def rms(xf, g):
    return (xf * lax.rsqrt(jnp.mean(xf * xf, axis=-1, keepdims=True) + EPS) * g).astype(jnp.bfloat16)


def dotf(a, b):
    return jnp.dot(a, b, preferred_element_type=jnp.float32)


def layer_kernel(n, cap, top,
                 x_hbm, idx_hbm, gate_ref, g1_hbm, g2_hbm, wq, wk, wv, wo, w1, w3, w2,
                 hv, moe_ref,
                 xv, idxv, g1v, g2v, bq, bk, bv, bo, e1, e3, e2,
                 xn, acc, part, tokv, dstv, toks, dsts,
                 rows32, zt, send, recv, xs, esend, back, moe32,
                 in_sem, w_sem, e_sem, s_sem, p_ssem, p_rsem, out_ssem, out_rsem, ret_ssem, ret_rsem):
    t2, d_model = xv.shape
    t_len = t2 // 2
    kb = d_model // LANES
    wid = wq.shape[1]
    cols = bq.shape[2]
    groups = wid // 2 // cols
    passes = cap // PAIR
    per = n // PARTS
    rows = per * PAIR
    first = torus_axes(n)[0][0]
    me = lax.axis_index('ep')
    own = [lax.rem(lax.div(me, stride), size) for size, stride in torus_axes(n)]
    core = lax.rem(me, 2)
    mate = me + 1 - 2 * core

    def weight_copies(g, slot):
        c = pl.ds(pl.multiple_of((core * groups + g) * cols, cols), cols)
        return [
            pltpu.make_async_copy(wq.at[:, c], bq.at[slot], w_sem.at[slot, 0]),
            pltpu.make_async_copy(wk.at[:, c], bk.at[slot], w_sem.at[slot, 1]),
            pltpu.make_async_copy(wv.at[:, c], bv.at[slot], w_sem.at[slot, 2]),
            pltpu.make_async_copy(wo.at[c, :], bo.at[slot], w_sem.at[slot, 3]),
        ]

    ins = [
        pltpu.make_async_copy(x_hbm, xv.at[:t_len], in_sem.at[0]),
        pltpu.make_async_copy(idx_hbm, idxv, in_sem.at[1]),
        pltpu.make_async_copy(g1_hbm, g1v, in_sem.at[2]),
        pltpu.make_async_copy(g2_hbm, g2v, in_sem.at[3]),
    ]
    for cp in ins:
        cp.start()
    for g in range(min(NBUF, groups)):
        for cp in weight_copies(g, g):
            cp.start()
    experts = [
        pltpu.make_async_copy(w1, e1, e_sem.at[0]),
        pltpu.make_async_copy(w3, e3, e_sem.at[1]),
        pltpu.make_async_copy(w2, e2, e_sem.at[2]),
    ]

    barrier = pltpu.get_barrier_semaphore()

    def hello(j, carry):
        pl.semaphore_signal(barrier, inc=1, device_id={'ep': j}, device_id_type=MESH)
        return carry

    lax.fori_loop(me + 1, n, hello, 0)
    lax.fori_loop(0, me, hello, 0)

    for cp in ins:
        cp.wait()
    exp = lax.broadcasted_iota(jnp.int32, (n, t_len), 0)
    member = jnp.zeros((n, t_len), jnp.float32)
    for j in range(top):
        member = member + (idxv[j:j + 1, :] == exp).astype(jnp.float32)
    before = lax.broadcasted_iota(jnp.int32, (t_len, t_len), 0) < lax.broadcasted_iota(jnp.int32, (t_len, t_len), 1)
    pos = dotf(member.astype(jnp.bfloat16), before.astype(jnp.bfloat16))
    off = number(n, [((exp // stride) % size + size - (me // stride) % size) % size
                     for size, stride in torus_axes(n)])
    nth = pos.astype(jnp.int32)
    place = (((nth // PAIR) * n + off) * PAIR + nth % PAIR).astype(jnp.float32)
    for j in range(top):
        hit = jnp.where(idxv[j:j + 1, :] == exp, place, 0.0)
        dstv[j:j + 1, :] = jnp.clip(jnp.sum(hit, axis=0, keepdims=True).astype(jnp.int32), 0, n * cap - 1)
    tok = lax.broadcasted_iota(jnp.int32, (n, t_len), 1).astype(jnp.float32)
    for c in range(cap):
        hit = jnp.where((member > 0) & (pos == c), tok, 0.0)
        tokv[:, c:c + 1] = jnp.clip(jnp.sum(hit, axis=1, keepdims=True).astype(jnp.int32), 0, t_len - 1)
    tables = [
        pltpu.make_async_copy(tokv, toks, s_sem.at[0]),
        pltpu.make_async_copy(dstv, dsts, s_sem.at[1]),
    ]
    for cp in tables:
        cp.start()

    xn[:t_len] = rms(xv[:t_len].astype(jnp.float32), g1v[...])
    acc[...] = jnp.zeros_like(acc)
    pl.semaphore_wait(barrier, n - 1)
    meet = pltpu.make_async_remote_copy(
        src_ref=xv.at[:t_len], dst_ref=xv.at[t_len:], send_sem=p_ssem.at[0], recv_sem=p_rsem.at[0],
        device_id={'ep': mate}, device_id_type=MESH)
    meet.start()
    meet.wait()
    xn[t_len:] = rms(xv[t_len:].astype(jnp.float32), g1v[...])
    row = lax.broadcasted_iota(jnp.int32, (t2, t2), 0)
    col = lax.broadcasted_iota(jnp.int32, (t2, t2), 1)
    keep = (row >= col) & (row // t_len == col // t_len)

    def group(g, carry):
        slot = g % NBUF
        for cp in weight_copies(g, slot):
            cp.wait()
        a = xn[...]
        q = dotf(a, bq[slot]).astype(jnp.bfloat16)
        k = dotf(a, bk[slot]).astype(jnp.bfloat16)
        v = dotf(a, bv[slot]).astype(jnp.bfloat16)
        outs = []
        for hd in range(cols // HEAD):
            c = slice(hd * HEAD, (hd + 1) * HEAD)
            sc = lax.dot_general(q[:, c], k[:, c], (((1,), (1,)), ((), ())),
                                 preferred_element_type=jnp.float32) * HEAD ** -0.5
            sc = jnp.where(keep, sc, -1e30)
            ex = jnp.exp(sc - jnp.max(sc, axis=-1, keepdims=True))
            p = (ex / jnp.sum(ex, axis=-1, keepdims=True)).astype(jnp.bfloat16)
            outs.append(dotf(p, v[:, c]).astype(jnp.bfloat16))
        o = jnp.concatenate(outs, axis=1)
        acc[...] += dotf(o, bo[slot])

        @pl.when(g + NBUF < groups)
        def _():
            for cp in weight_copies(g + NBUF, slot):
                cp.start()

        @pl.when(g == max(groups - 2, 0))
        def _():
            for cp in experts:
                cp.start()

        return carry

    lax.fori_loop(0, groups, group, 0)

    swap = pltpu.make_async_remote_copy(
        src_ref=acc.at[t_len:], dst_ref=part, send_sem=p_ssem.at[1], recv_sem=p_rsem.at[1],
        device_id={'ep': mate}, device_id_type=MESH)
    swap.start()
    swap.wait()
    att = (acc[:t_len] + part[...]).astype(jnp.bfloat16)
    h = (xv[:t_len].astype(jnp.float32) + att.astype(jnp.float32)).astype(jnp.bfloat16)
    hv[...] = h
    z = rms(h.astype(jnp.float32), g2v[...]).astype(jnp.float32)
    for b in range(kb):
        rows32[:t_len, b, :] = z[:, b * LANES:(b + 1) * LANES]
    zt[...] = rows32[:t_len].astype(jnp.bfloat16)
    for cp in tables:
        cp.wait()

    for p in range(passes):
        for c in range(PAIR):
            recv[p * n * PAIR + c] = zt[toks[me, p * PAIR + c]]

    def block(p, i):
        return pl.ds((p * n + i) * PAIR, PAIR)

    def fill(p, q, a):
        d = peer(n, own, q, a, 1)
        for c in range(PAIR):
            send[(p * n + first * q + a) * PAIR + c] = zt[toks[d, p * PAIR + c]]

    def out_copy(p, q, a):
        i = first * q + a
        return pltpu.make_async_remote_copy(
            src_ref=send.at[block(p, i)], dst_ref=recv.at[block(p, i)],
            send_sem=out_ssem.at[p], recv_sem=out_rsem.at[p * PARTS + lax.div(i, per)],
            device_id={'ep': peer(n, own, q, a, 1)}, device_id_type=MESH)

    quads = n // first
    for p in range(passes):
        for a in range(first):
            fill(p, 0, a)

        def dispatch(q, carry):
            for a in range(first):
                fill(p, q, a)
            for a in range(first):
                if a == 0:
                    @pl.when(q > 1)
                    def _():
                        out_copy(p, q - 1, a).start()
                else:
                    out_copy(p, q - 1, a).start()
            return carry

        lax.fori_loop(1, quads, dispatch, 0)
        for a in range(first):
            out_copy(p, quads - 1, a).start()

    for cp in experts:
        cp.wait()

    def span(lo, count, src, dst, ssem, rsem):
        blk = pl.ds(lo, count)
        return pltpu.make_async_remote_copy(
            src_ref=src.at[blk], dst_ref=dst.at[blk], send_sem=ssem, recv_sem=rsem,
            device_id={'ep': mate}, device_id_type=MESH)

    def ret_copy(p, q, a):
        i = first * q + a
        return pltpu.make_async_remote_copy(
            src_ref=esend.at[block(p, i)], dst_ref=back.at[block(p, i)],
            send_sem=ret_ssem.at[p], recv_sem=ret_rsem.at[p],
            device_id={'ep': peer(n, own, q, a, -1)}, device_id_type=MESH)

    def chunk(ch, carry):
        p = lax.div(ch, PARTS)
        half = lax.rem(ch, PARTS)
        base = ch * rows

        @pl.when(half == 0)
        def _():
            span(base + PAIR, rows - PAIR, send, recv, out_ssem.at[0], out_rsem.at[ch]).wait_recv()

        @pl.when(half > 0)
        def _():
            span(base, rows, send, recv, out_ssem.at[0], out_rsem.at[ch]).wait_recv()

        rows32[:rows] = recv[pl.ds(base, rows)].astype(jnp.float32)
        for b in range(kb):
            xs[:, b * LANES:(b + 1) * LANES] = rows32[:rows, b, :].astype(jnp.bfloat16)
        r = xs[...]
        h1 = dotf(r, e1[...])
        h3 = dotf(r, e3[...])
        u = (jax.nn.silu(h1) * h3).astype(jnp.bfloat16)
        eo = dotf(u, e2[...])
        for b in range(kb):
            rows32[:rows, b, :] = eo[:, b * LANES:(b + 1) * LANES]
        esend[pl.ds(base, rows)] = rows32[:rows].astype(jnp.bfloat16)

        @pl.when(half == 0)
        def _():
            back[pl.ds(base, PAIR)] = esend[pl.ds(base, PAIR)]

        def give(k, c2):
            q = half * (quads // PARTS) + k
            for a in range(first):
                if a == 0:
                    @pl.when(q > 0)
                    def _():
                        ret_copy(p, q, a).start()
                else:
                    ret_copy(p, q, a).start()
            return c2

        lax.fori_loop(0, quads // PARTS, give, 0)
        return carry

    lax.fori_loop(0, passes * PARTS, chunk, 0)

    def full(p, src, dst, ssem, rsem):
        return span((p * n + 1) * PAIR, (n - 1) * PAIR, src, dst, ssem, rsem)

    for p in range(passes):
        full(p, esend, back, ret_ssem.at[p], ret_rsem.at[p]).wait_recv()

    def combine(k, carry):
        for s in range(4):
            t = 4 * k + s
            total = jnp.zeros((kb, LANES), jnp.float32)
            for j in range(top):
                total = total + back[dsts[j, t]].astype(jnp.float32) * gate_ref[j, t]
            moe32[t] = total
        return carry

    lax.fori_loop(0, t_len // 4, combine, 0)
    for b in range(kb):
        moe_ref[:, b * LANES:(b + 1) * LANES] = moe32[:, b, :]

    for p in range(passes):
        full(p, send, recv, out_ssem.at[p], out_rsem.at[0]).wait_send()
        full(p, esend, back, ret_ssem.at[p], ret_rsem.at[p]).wait_send()


def layer(n, x, idx, gates, g1, g2, wq, wk, wv, wo, w1, w3, w2):
    t_len, d = x.shape
    top = idx.shape[0]
    avg = top * t_len // n
    cap = avg + avg // 2
    cols = min(COLS, wq.shape[1] // 2)
    kb = d // LANES
    ff = w1.shape[1]
    passes = cap // PAIR
    rows = n // PARTS * PAIR
    bf, f32, i32 = jnp.bfloat16, jnp.float32, jnp.int32
    anyspec = pl.BlockSpec(memory_space=pl.ANY)
    V, DMA = pltpu.VMEM, pltpu.SemaphoreType.DMA
    return pl.pallas_call(
        functools.partial(layer_kernel, n, cap, top),
        out_shape=(jax.ShapeDtypeStruct((t_len, d), bf), jax.ShapeDtypeStruct((t_len, d), f32)),
        in_specs=[anyspec, anyspec, pl.BlockSpec(memory_space=pltpu.SMEM)] + [anyspec] * 9,
        out_specs=(pl.BlockSpec(memory_space=pltpu.VMEM), pl.BlockSpec(memory_space=pltpu.VMEM)),
        scratch_shapes=[
            V((2 * t_len, d), bf), V((top, t_len), i32), V((1, d), f32), V((1, d), f32),
            V((NBUF, d, cols), bf), V((NBUF, d, cols), bf), V((NBUF, d, cols), bf), V((NBUF, cols, d), bf),
            V((d, ff), bf), V((d, ff), bf), V((ff, d), bf),
            V((2 * t_len, d), bf), V((2 * t_len, d), f32), V((t_len, d), f32),
            V((n, cap), i32), V((top, t_len), i32), pltpu.SMEM((n, cap), i32), pltpu.SMEM((top, t_len), i32),
            V((max(rows, t_len), kb, LANES), f32), V((t_len, kb, LANES), bf),
            V((n * cap, kb, LANES), bf), V((n * cap, kb, LANES), bf), V((rows, d), bf),
            V((n * cap, kb, LANES), bf), V((n * cap, kb, LANES), bf), V((t_len, kb, LANES), f32),
            DMA((4,)), DMA((NBUF, 4)), DMA((3,)), DMA((2,)), DMA((2,)), DMA((2,)),
            DMA((passes,)), DMA((passes * PARTS,)), DMA((passes,)), DMA((passes,)),
        ],
        compiler_params=pltpu.CompilerParams(
            collective_id=0, has_side_effects=True, vmem_limit_bytes=67043328),
        name='layer',
    )(x, idx, gates, g1, g2, wq, wk, wv, wo, w1, w3, w2)


def solution(mesh):
    n = mesh.shape['ep']
    tok = P(('dp', 'ep'))
    rep = P()
    exs = P('ep')

    def body(x, idx, gates, g1, wq, wk, wv, wo, g2, w1, w3, w2):
        d = x.shape[-1]
        h, moe = layer(n, x[0], idx[0].T, gates[0].T, g1.reshape(1, d), g2.reshape(1, d),
                  wq, wk, wv, wo, w1[0], w3[0], w2[0])
        return (h.astype(jnp.float32) + moe).astype(jnp.bfloat16)[None]

    return jax.shard_map(body, mesh=mesh, in_specs=(tok, tok, tok, rep, rep, rep, rep, rep, rep, exs, exs, exs), out_specs=tok, check_vma=False)
```
